128 devices in a mesh: section: 16 (over x_lo, y, core), tensor: 4 (over z), dp: 2 (over x_hi).
Axes of the slice: x: 4 (x_hi: 2, x_lo: 2; x = x_hi * 2 + x_lo), y: 4, z: 4, core: 2. Of those that a mesh axis runs over, the one named last changes fastest.
Arguments:
- section_up: bfloat16 [16, 4096, 7168], P('section', 'dp', 'tensor'), may hold values from -0.09375 to 0.09375
- section_down: bfloat16 [16, 4096, 7168], P('section', 'dp', 'tensor'), may hold values from -0.0625 to 0.0625
- backup_up: bfloat16 [2, 16, 4, 32, 7168], P('dp', 'section', 'tensor'), may hold values from -0.09375 to 0.09375
- backup_down: bfloat16 [2, 16, 4, 32, 7168], P('dp', 'section', 'tensor'), may hold values from -0.0625 to 0.0625
- norm_gain: float32 [16, 4096], P('section'), may hold values from 0.25 to 1.75
- micro_batches: bfloat16 [16, 64, 4096], P(None, 'dp', 'tensor'), may hold values from -24 to 24
- failed_section: int32 [1], replicated, may hold values from 0 to 1048575
- live_batches: int32 [1], replicated, may hold values from 0 to 589823
Outputs:
- finals: bfloat16 [16, 64, 4096], P('section', 'dp', 'tensor')
The draws below stay inside these ranges and needn't reach their ends.
Inputs may be any that keep to these rules, and one draw needn't show every extreme that they name: failed_section modulo the number of sections names the failed section. micro-batches 0 to 16 // 2 + (live_batches modulo (16 - 16 // 2 + 1)) - 1 run.
All inputs are finite; a program needn't handle non-finite values.
Results may differ from the reference program's by a relative error of at most 0.03.
Values may be sent and summed in bfloat16 or wider, within the bound.
No kernel may reach another device: no remote copies, remote signals or barrier semaphores. Data moves between devices by JAX's collectives and lax.ppermute only.
A program may use at most 192 MiB of HBM per device.

```python
import math
import jax
import jax.numpy as jnp
from jax import lax

D = 4096
FF = 7168
MB = 16
TOKENS_MB = 64
ROWS_PIECE = 32
N_SECTION = 16
N_TENSOR = 4
N_DP = 2


def draw_micro_batches(key, part):
    first, second, third = jax.random.split(key, 3)
    shape = (MB, TOKENS_MB, D)
    row_scale = jnp.exp(jax.random.uniform(second, (MB, TOKENS_MB, 1), jnp.float32, math.log(0.3), math.log(3.0)))
    column_scale = jnp.exp(jax.random.uniform(third, (1, 1, D), jnp.float32, math.log(0.3), math.log(3.0)))
    values = jax.random.normal(first, shape, jnp.float32) * row_scale * column_scale
    return jnp.clip(values, -24.0, 24.0).astype(jnp.bfloat16)


def shard_levels(rng, extent, pieces, smallest, top_value):
    factor_of = 1.0
    for dim, shards_of in pieces:
        draws = jax.random.uniform(jax.random.fold_in(jax.random.fold_in(rng, 6), dim), (shards_of,), jnp.float32, smallest / len(pieces), top_value / len(pieces))
        factor_of = factor_of * jnp.repeat(jnp.exp(draws), extent[dim] // shards_of).reshape((-1,) + (1,) * (len(extent) - 1 - dim))
    return factor_of


def gaussian(key, shape, deviation, limit, shards=(), kind=jnp.bfloat16):
    entries = jax.random.normal(key, shape, jnp.float32) * deviation
    if len(shards) > 0:
        entries = shard_levels(key, shape, shards, -0.22, 0.18) * entries
    return jnp.clip(entries, min=-limit, max=limit).astype(kind)


def setup_inputs(seed: int = 0) -> dict:
    key_of = jax.random.split(jax.random.key(seed), 9)
    section_up = gaussian(key_of[0], (N_SECTION, D, FF), D ** -0.5, 0.09375, ((0, 16), (1, 2), (2, 4)))
    section_down = gaussian(key_of[1], (N_SECTION, D, FF), FF ** -0.5, 0.0625, ((0, 16), (1, 2), (2, 4)))
    backup_up = gaussian(key_of[2], (N_DP, N_SECTION, N_TENSOR, ROWS_PIECE, FF), D ** -0.5, 0.09375, ((0, 2), (1, 16), (2, 4)))
    backup_down = gaussian(key_of[3], (N_DP, N_SECTION, N_TENSOR, ROWS_PIECE, FF), FF ** -0.5, 0.0625, ((0, 2), (1, 16), (2, 4)))
    norm_gain = jnp.clip(1.0 + 0.15 * jax.random.normal(key_of[4], (N_SECTION, D), jnp.float32), 0.25, 1.75)
    micro_batches = draw_micro_batches(jax.random.fold_in(key_of[8], 71), 0)
    failed_section = jax.random.randint(key_of[6], (1,), 0, N_SECTION * 65536).astype(jnp.int32)
    live_batches = jax.random.randint(key_of[7], (1,), 0, 65536 * (MB - MB // 2 + 1)).astype(jnp.int32)
    return dict(section_up=section_up, section_down=section_down, backup_up=backup_up, backup_down=backup_down, norm_gain=norm_gain, micro_batches=micro_batches, failed_section=failed_section, live_batches=live_batches)


def reference(section_up, section_down, backup_up, backup_down, norm_gain, micro_batches, failed_section, live_batches):
    failed = failed_section[0] % N_SECTION
    live_count = MB // 2 + live_batches[0] % (MB - MB // 2 + 1)
    spare_up = backup_up.reshape(D, FF)
    spare_down = backup_down.reshape(D, FF)
    batch_index = lax.broadcasted_iota(jnp.int32, (MB, 1, 1), 0)
    inputs = jnp.where(batch_index < live_count, micro_batches, jnp.zeros_like(micro_batches))
    state_rows = inputs.reshape(MB * TOKENS_MB, D)
    block_width = FF // N_TENSOR

    def one_section(carried, section_layer):
        up_weight, down_weight, gain_row, section_index = section_layer
        chosen_up = jnp.where(section_index == failed, spare_up, up_weight)
        chosen_down = jnp.where(section_index == failed, spare_down, down_weight)
        values = carried.astype(jnp.float32)
        mean_square = lax.optimization_barrier(jnp.mean(values * values, axis=1, keepdims=True))
        normed = (values * lax.rsqrt(mean_square + 1e-05) * gain_row).astype(jnp.bfloat16)
        hidden = jax.nn.silu(jnp.dot(normed, chosen_up, preferred_element_type=jnp.float32)).astype(jnp.bfloat16)
        down_total = jnp.zeros((carried.shape[0], D), jnp.float32)
        for block_index in range(N_TENSOR):
            lower = block_index * block_width
            block_term = lax.dot_general(hidden[:, lower:lower + block_width], chosen_down[:, lower:lower + block_width], (((1,), (1,)), ((), ())), preferred_element_type=jnp.float32)
            down_total = down_total + lax.optimization_barrier(block_term.astype(jnp.bfloat16)).astype(jnp.float32)
        return ((values + down_total).astype(jnp.bfloat16), None)
    indices = jnp.arange(N_SECTION, dtype=jnp.int32)
    final_rows, _ = lax.scan(one_section, state_rows, (section_up, section_down, norm_gain, indices))
    return final_rows.reshape(MB, TOKENS_MB, D)
```

```python
import jax
import jax.numpy as jnp
from jax import lax
from jax.sharding import PartitionSpec as P


def flip_low(t):
    return t ^ 1


def flip_all(t):
    return 3 - t


def same(t):
    return t


def across_tensor(x, partner):
    return lax.ppermute(x, "tensor", [(t, partner(t)) for t in range(lax.axis_size("tensor"))])


def to_next(x, partner):
    sections, width = (lax.axis_size("section"), lax.axis_size("tensor"))
    route = [
        (s * width + t, ((s + 1) % sections) * width + partner(t))
        for s in range(sections)
        for t in range(width)
    ]
    return lax.ppermute(x, ("section", "tensor"), route)


def across_dp(x):
    return lax.ppermute(x, "dp", [(0, 1), (1, 0)])


def corner_swap(x, dp_number, tensor_number):
    width = lax.axis_size("tensor")
    route = []
    for d in range(2):
        for t in range(width):
            target = (t // 2, 2 * d + t % 2)
            if target != (d, t):
                route.append((t * 2 + d, target[1] * 2 + target[0]))
    moved = lax.ppermute(x, ("tensor", "dp"), route)
    return jnp.where(tensor_number // 2 == dp_number, x, moved)


def rebuilt(backup):
    rows, full = backup.shape[-2:]
    width = lax.axis_size("tensor")
    blocks = jnp.moveaxis(backup.reshape(rows, width, full // width), 1, 0)
    return blocks


def body(
    section_up,
    section_down,
    backup_up,
    backup_down,
    norm_gain,
    micro_batches,
    failed_section,
    live_batches,
):
    f32, bf16 = (jnp.float32, jnp.bfloat16)
    section_number = lax.axis_index("section")
    tensor_number = lax.axis_index("tensor")
    dp_number = lax.axis_index("dp")
    section_count = lax.axis_size("section")
    batch_count, tok_rows, share = micro_batches.shape
    half_width, block_width = section_up.shape[1:]
    full_width = half_width * 2
    live_count = batch_count // 2 + live_batches[0] % (batch_count - batch_count // 2 + 1)

    own_piece = corner_swap(micro_batches, dp_number, tensor_number)
    pieces = lax.all_gather(own_piece, "tensor", axis=0)
    pieces = pieces.reshape(2, 2, batch_count, tok_rows, share)
    entering = pieces.transpose(2, 0, 3, 1, 4).reshape(batch_count, 2 * tok_rows, half_width)

    both = jnp.stack([rebuilt(backup_up), rebuilt(backup_down)], axis=1)
    swapped = lax.all_to_all(both, "tensor", 0, 0, tiled=True)
    spare_up = lax.all_gather(swapped[:, 0].reshape(-1, block_width), "section", axis=0, tiled=True)
    spare_down = lax.all_gather(swapped[:, 1].reshape(-1, block_width), "section", axis=0, tiled=True)
    is_failed = section_number == failed_section[0] % section_count
    up = jnp.where(is_failed, spare_up, section_up[0])
    down = jnp.where(is_failed, spare_down, section_down[0])
    gain = lax.dynamic_slice_in_dim(norm_gain[0], dp_number * half_width, half_width)[None, :]

    def tick(tick_index, state):
        first, second, collected = state
        arrived = (first.astype(f32) + second.astype(f32)).astype(bf16)
        slot = jnp.clip(tick_index - section_count, 0, batch_count - 1)
        collected = lax.dynamic_update_index_in_dim(collected, arrived, slot, 0)
        picked = lax.dynamic_index_in_dim(
            entering, jnp.minimum(tick_index, batch_count - 1), 0, keepdims=False
        )
        picked = jnp.where(tick_index < live_count, picked, jnp.zeros_like(picked))
        rows = jnp.where(section_number == 0, picked, arrived)
        values = rows.astype(f32)
        squares = jnp.sum(values * values, axis=1, keepdims=True)
        scaled = (values * gain).astype(bf16)
        pre = jnp.dot(scaled, up, preferred_element_type=f32).astype(bf16)
        coarse = squares.astype(bf16)
        fine = (squares - coarse.astype(f32)).astype(bf16)
        ones = jnp.ones((1, 64), bf16)
        message = jnp.concatenate([pre, coarse * ones, fine * ones], axis=1)
        other = across_dp(message)
        other_squares = other[:, block_width : block_width + 1].astype(f32) + other[
            :, block_width + 64 : block_width + 65
        ].astype(f32)
        scale = lax.rsqrt((squares + other_squares) / full_width + 1e-05)
        total = (pre.astype(f32) + other[:, :block_width].astype(f32)) * scale
        hidden = jax.nn.silu(total).astype(bf16)
        part = lax.dot_general(
            hidden, down, (((1,), (1,)), ((), ())), preferred_element_type=f32
        ).astype(bf16)
        quarter = half_width // 2
        left, right = (part[:, :quarter], part[:, quarter:])
        left = (left.astype(f32) + across_tensor(left, flip_low).astype(f32)).astype(bf16)
        right = (right.astype(f32) + across_tensor(right, flip_all).astype(f32)).astype(bf16)
        pair = jnp.concatenate([left, right], axis=1)
        kept = (values + pair.astype(f32)).astype(bf16)
        first = to_next(kept, same)
        second = jnp.concatenate([to_next(left, flip_all), to_next(right, flip_low)], axis=1)
        return (first, second, collected)

    nothing = jnp.zeros((2 * tok_rows, half_width), bf16)
    store = jnp.zeros((batch_count, 2 * tok_rows, half_width), bf16)
    first, second, collected = lax.fori_loop(
        0, live_count + section_count - 1, tick, (nothing, nothing, store)
    )
    arrived = (first.astype(f32) + second.astype(f32)).astype(bf16)
    collected = lax.dynamic_update_index_in_dim(collected, arrived, live_count - 1, 0)

    piece = lax.dynamic_slice(
        collected,
        (0, (tensor_number // 2) * tok_rows, (tensor_number % 2) * share),
        (batch_count, tok_rows, share),
    )
    step = section_count // 2
    while step:
        route = [(s, s + step) for s in range(0, section_count, 2 * step)]
        moved = lax.ppermute(piece[step:], "section", route)
        piece = jnp.where((section_number & step) != 0, moved, piece[:step])
        step //= 2
    return corner_swap(piece, dp_number, tensor_number)


def solution(mesh):
    placed = (
        P("section", "dp", "tensor"),
        P("section", "dp", "tensor"),
        P("dp", "section", "tensor", None, None),
        P("dp", "section", "tensor", None, None),
        P("section", None),
        P(None, "dp", "tensor"),
        P(),
        P(),
    )
    return jax.shard_map(
        body, mesh=mesh, in_specs=placed, out_specs=P("section", "dp", "tensor"), check_vma=False
    )
```
